32 devices in a mesh: member: 2 (over y), tx: 4 (over z), ty: 4 (over x, core).
Axes of the slice: x: 2, y: 2, z: 4, core: 2. Of those that a mesh axis runs over, the one named last changes fastest.
Arguments:
- tracers: float32 [80, 3, 128, 512], P('member', None, 'tx', 'ty'), parts along dimension 0, may hold values from 0.05 to 2
- velocity: float32 [2, 3, 128, 512], P(None, None, 'tx', 'ty'), may hold values from -0.4 to 0.4
- land_mask: int32 [3, 128, 512], P(None, 'tx', 'ty'), may hold values 0 or 1
- sunlight: float32 [128, 512], P('tx', 'ty'), may hold values from 0.3 to 3
- growth_max: float32 [52], P('member'), parts along dimension 0, may hold values from 0.2 to 1.5
- half_sat: float32 [8, 26], P('member'), parts along dimension 0, may hold values from 0.05 to 1
- light_half: float32 [52], P('member'), parts along dimension 0, may hold values from 0.1 to 1
- graze_max: float32 [20], P('member'), parts along dimension 0, may hold values from 0.2 to 1.5
- graze_half: float32 [20], P('member'), parts along dimension 0, may hold values from 0.2 to 2
- palatable: int32 [20, 26], P('member'), parts along dimension 0, may hold values 0 or 1
- stoichiometry: float32 [4], replicated, may hold values from 0.05 to 1
Outputs:
- updated: float32 [80, 3, 128, 512], P('member', None, 'tx', 'ty'), parts along dimension 0
The draws below stay inside these ranges and needn't reach their ends.
There are 2 independent parts, one for each index of `member`. The reference program is written for one: setup_inputs(seed, part) draws one part's arguments, and reference() takes and returns one part's arrays. A program takes and returns all parts, laid end to end along the dimension named above; an argument that names none is the same for every part. Nothing has to cross between parts.
All inputs are finite; a program needn't handle non-finite values. No bound on the sum of `land_mask` on one device may be relied on, other than what follows from the above.
Results may differ from the reference program's by a relative error of at most 0.000064.
Values sent between devices are 32-bit elements; how exact they have to be, the bound alone decides.
A program may use at most 64 MiB of HBM per device.

```python
import math
import jax
import jax.numpy as jnp
from jax import lax

NNUT = 4
NPHY = 26
NZOO = 10
NR = 3
NTR = 40
NX = 128
NY = 512


def with_ends(entries, rng, least, high):
    dims = entries.shape
    spot = [jax.random.randint(jax.random.fold_in(rng, axis), (), 0, dims[axis]) for axis in range(len(dims))]
    entries = entries.at[tuple(spot)].set(least)
    longest = dims.index(max(dims))
    spot[longest] = (spot[longest] + 1) % dims[longest]
    return entries.at[tuple(spot)].set(high)


def block_scale(own_key, dims, cuts, low, largest):
    loudness = 1.0
    for dim, blocks in cuts:
        steps = jax.random.uniform(jax.random.fold_in(jax.random.fold_in(own_key, 6), dim), (blocks,), jnp.float32, low / len(cuts), largest / len(cuts))
        loudness = loudness * jnp.repeat(jnp.exp(steps), dims[dim] // blocks).reshape((-1,) + (1,) * (len(dims) - 1 - dim))
    return loudness


def setup_inputs(seed: int = 0, part: int = 0) -> dict:
    keys = jax.random.split(jax.random.key(seed), 12)
    own_keys = jax.random.split(jax.random.fold_in(keys[11], part), 12)
    tracers = jnp.clip(jnp.exp(math.log(2.0) - 3.6888794 * jax.random.uniform(own_keys[0], (NTR, NR, NX, NY), jnp.float32) ** block_scale(own_keys[0], (NTR, NR, NX, NY), ((2, 4), (3, 4)), -0.2, 0.2)), 0.05, 2.0)
    velocity = jnp.clip(jax.random.uniform(keys[1], (2, NR, NX, NY), jnp.float32, -0.4, 0.4) * block_scale(keys[1], (2, NR, NX, NY), ((2, 4), (3, 4)), -0.4, 0.0), -0.4, 0.4)
    land_mask = with_ends((jax.random.randint(keys[2], (NR, NX, NY), 0, 5) < 4).astype(jnp.int32), jax.random.fold_in(keys[2], 1), 0, 1)
    sunlight = jnp.clip(jnp.exp(math.log(3.0) - 2.3025851 * jax.random.uniform(keys[3], (NX, NY), jnp.float32) ** block_scale(keys[3], (NX, NY), ((0, 4), (1, 4)), -0.2, 0.2)), 0.3, 3.0)
    growth_max = jnp.clip(jnp.exp(jax.random.uniform(own_keys[4], (NPHY,), jnp.float32, math.log(0.2), math.log(1.5))), 0.2, 1.5)
    half_sat = jnp.clip(jnp.exp(jax.random.uniform(own_keys[5], (NNUT, NPHY), jnp.float32, math.log(0.05), math.log(1.0))), 0.05, 1.0)
    light_half = jnp.clip(jnp.exp(jax.random.uniform(own_keys[6], (NPHY,), jnp.float32, math.log(0.1), math.log(1.0))), 0.1, 1.0)
    graze_max = jnp.clip(jnp.exp(jax.random.uniform(own_keys[7], (NZOO,), jnp.float32, math.log(0.2), math.log(1.5))), 0.2, 1.5)
    graze_half = jnp.clip(jnp.exp(jax.random.uniform(own_keys[8], (NZOO,), jnp.float32, math.log(0.2), math.log(2.0))), 0.2, 2.0)
    palatable = with_ends((jax.random.randint(own_keys[9], (NZOO, NPHY), 0, 2) < 1).astype(jnp.int32), jax.random.fold_in(own_keys[9], 1), 0, 1)
    stoichiometry = jnp.clip(jnp.exp(jax.random.uniform(keys[10], (NNUT,), jnp.float32, math.log(0.05), math.log(1.0))), 0.05, 1.0)
    return dict(tracers=tracers, velocity=velocity, land_mask=land_mask, sunlight=sunlight, growth_max=growth_max, half_sat=half_sat, light_half=light_half, graze_max=graze_max, graze_half=graze_half, palatable=palatable, stoichiometry=stoichiometry)


plankton_mortality = 0.05
grazer_mortality = 0.3
assimilation = 0.3
attenuation = 0.4


def window(values, offset, amount, axis_dim):
    return lax.slice_in_dim(values, offset, offset + amount, axis=axis_dim)


def advect(padded, courant, wet_mask, axis_dim, length):
    face_count = length + 1
    far_left = window(padded, 0, face_count, axis_dim)
    near_left = window(padded, 1, face_count, axis_dim)
    near_right = window(padded, 2, face_count, axis_dim)
    far_right = window(padded, 3, face_count, axis_dim)
    opened = window(wet_mask, 1, face_count, axis_dim) * window(wet_mask, 2, face_count, axis_dim)
    transport = window(courant, 2, face_count, axis_dim) * opened
    face_flux = transport * ((7.0 / 12.0) * (near_left + near_right) - (1.0 / 12.0) * (far_left + far_right))
    face_flux = face_flux + jnp.abs(transport) * (1.0 / 12.0) * (far_right - 3.0 * near_right + 3.0 * near_left - far_left)
    centre = window(padded, 2, length, axis_dim)
    outflow = window(face_flux, 1, length, axis_dim) - window(face_flux, 0, length, axis_dim)
    spread = window(transport, 1, length, axis_dim) - window(transport, 0, length, axis_dim)
    return centre - outflow + centre * spread


def ecology(concentration, irradiance, growth_max, half_sat, light_half, graze_max, graze_half, palatable, stoichiometry):
    nutrients = concentration[:NNUT]
    phytoplankton = concentration[NNUT:NNUT + NPHY]
    zooplankton = concentration[NNUT + NPHY:]
    saturation = nutrients[:, None, :] / (nutrients[:, None, :] + half_sat[:, :, None])
    nutrient_limit = jnp.min(saturation, axis=0)
    light_limit = irradiance[None, :] / (irradiance[None, :] + light_half[:, None])
    growth = growth_max[:, None] * nutrient_limit * light_limit * phytoplankton
    prey_weights = palatable.astype(jnp.float32)
    available = jnp.dot(prey_weights, phytoplankton, precision=lax.Precision.HIGHEST)
    grazing_rate = graze_max[:, None] * zooplankton / (graze_half[:, None] + available)
    grazed = phytoplankton * jnp.dot(prey_weights.T, grazing_rate, precision=lax.Precision.HIGHEST)
    ingested = grazing_rate * available
    plankton_loss = plankton_mortality * phytoplankton
    grazer_loss = grazer_mortality * zooplankton * zooplankton
    phyto_change = growth - grazed - plankton_loss
    grazer_change = assimilation * ingested - grazer_loss
    recycled = jnp.sum(plankton_loss, axis=0) + jnp.sum(grazer_loss, axis=0) + (1.0 - assimilation) * jnp.sum(ingested, axis=0) - jnp.sum(growth, axis=0)
    nutrient_change = stoichiometry[:, None] * recycled[None, :]
    return jnp.concatenate([nutrient_change, phyto_change, grazer_change], axis=0)


def reference(tracers, velocity, land_mask, sunlight, growth_max, half_sat, light_half, graze_max, graze_half, palatable, stoichiometry):
    def pad_along(values):
        return jnp.pad(values, ((0, 0), (0, 0), (2, 2), (0, 0)), mode="wrap")

    def pad_across(values):
        return jnp.pad(values, ((0, 0), (0, 0), (0, 0), (2, 2)))

    def one_layer(layer_index):
        concentration = lax.dynamic_slice_in_dim(tracers, layer_index, 1, 1)
        flow = lax.dynamic_slice_in_dim(velocity, layer_index, 1, 1)
        wet_mask = lax.dynamic_slice_in_dim(land_mask, layer_index, 1, 0).astype(jnp.float32)[None]
        after_along = advect(pad_along(concentration), pad_along(flow[0:1]), pad_along(wet_mask), 2, NX)
        advected = advect(pad_across(after_along), pad_across(flow[1:2]), pad_across(wet_mask), 3, NY)
        depth_factor = jnp.exp(-attenuation * (layer_index.astype(jnp.float32) + 0.5))
        irradiance = (sunlight * depth_factor).reshape(-1)
        tendency = ecology(concentration.reshape(NTR, -1), irradiance, growth_max, half_sat, light_half, graze_max, graze_half, palatable, stoichiometry)
        return advected + wet_mask * tendency.reshape(concentration.shape)

    layers = lax.map(one_layer, jnp.arange(NR, dtype=jnp.int32))
    return jnp.moveaxis(layers[:, :, 0], 0, 1)
```

```python
import functools

import jax
import jax.numpy as jnp
from jax import lax
from jax.experimental import pallas as pl
from jax.experimental.pallas import tpu as pltpu
from jax.sharding import PartitionSpec as P

NNUT = 4
plankton_mortality = 0.05
grazer_mortality = 0.3
assimilation = 0.3
attenuation = 0.4

ROWS = 8
LANES = 128
FIRST = 8
GROUP = 4
PER = LANES // GROUP
MESH = pl.DeviceIdType.MESH


def stencil_weights(here, after):
    hp, hm = jnp.maximum(here, 0.0), jnp.minimum(here, 0.0)
    ap, am = jnp.maximum(after, 0.0), jnp.minimum(after, 0.0)
    sixth = 1.0 / 6.0
    return (
        -sixth * hp,
        5.0 * sixth * hp + 2.0 * sixth * hm + sixth * ap,
        1.0 - 4.0 * sixth * hp - sixth * hm + sixth * ap + 4.0 * sixth * am,
        -sixth * hm - 2.0 * sixth * ap - 5.0 * sixth * am,
        sixth * am,
    )


def exchange_kernel(
    dims,
    tracers,
    velocity,
    land_mask,
    sunlight,
    growth_max,
    half_sat,
    light_half,
    graze_max,
    graze_half,
    palatable,
    stoichiometry,
    swept,
    tend,
    halo,
    pad,
    mask_buf,
    sun_buf,
    send_lo,
    send_hi,
    recv_lo,
    recv_hi,
    pack_in,
    pack_out,
    left_in,
    left_out,
    right_in,
    right_out,
    prey,
    load_sems,
    row_sems,
    col_sems,
):
    count, levels, along, nphy, nzoo = dims
    fields = count + 2
    tiles = along // ROWS
    inner = tiles - 2
    last = FIRST + along - ROWS
    tx_size, ty_size = lax.axis_size("tx"), lax.axis_size("ty")
    tx, ty = lax.axis_index("tx"), lax.axis_index("ty")
    up, down = lax.rem(tx + 1, tx_size), lax.rem(tx + tx_size - 1, tx_size)
    right, left = lax.rem(ty + 1, ty_size), lax.rem(ty + ty_size - 1, ty_size)

    def load(slot, src, dst):
        copy = pltpu.make_async_copy(src, dst, load_sems.at[slot])
        copy.start()
        return copy

    own = pl.ds(0, count)
    loads = [
        load(0, land_mask, mask_buf),
        load(1, velocity.at[0], pad.at[count, :, pl.ds(FIRST, along), :]),
        load(2, tracers.at[:, :, pl.ds(0, ROWS), :], pad.at[own, :, pl.ds(FIRST, ROWS), :]),
        load(3, tracers.at[:, :, pl.ds(along - ROWS, ROWS), :], pad.at[own, :, pl.ds(last, ROWS), :]),
        load(4, tracers.at[:, :, pl.ds(ROWS, along - 2 * ROWS), :],
             pad.at[own, :, pl.ds(FIRST + ROWS, along - 2 * ROWS), :]),
        load(5, velocity.at[1], pad.at[count + 2, :, pl.ds(FIRST, along), :]),
        load(6, sunlight, sun_buf),
    ]

    barrier = pltpu.get_barrier_semaphore()
    for target in ({"tx": up}, {"tx": down}, {"ty": right}, {"ty": left}):
        pl.semaphore_signal(barrier, inc=1, device_id=target, device_id_type=MESH)

    def to_float(z, carry):
        for k in range(nphy):
            prey[z, k] = palatable[z, k].astype(jnp.float32)
        return carry

    lax.fori_loop(0, nzoo, to_float, 0)

    loads[0].wait()
    pad[count + 1, :, FIRST:FIRST + along, :] = mask_buf[...].astype(jnp.float32)
    for slot in (1, 2, 3):
        loads[slot].wait()
    send_lo[...] = pad[0:fields, :, FIRST:FIRST + 2, :]
    send_hi[...] = pad[0:fields, :, FIRST + along - 2:FIRST + along, :]

    pl.semaphore_wait(barrier, 4)

    def remote(src, dst, sems, slot, target):
        return pltpu.make_async_remote_copy(
            src_ref=src, dst_ref=dst, send_sem=sems.at[slot, 0], recv_sem=sems.at[slot, 1],
            device_id=target, device_id_type=MESH,
        )

    to_down = remote(send_lo, recv_hi, row_sems, 0, {"tx": down})
    to_up = remote(send_hi, recv_lo, row_sems, 1, {"tx": up})
    to_down.start()
    to_up.start()
    for slot in (4, 5, 6):
        loads[slot].wait()

    lane_group = lax.broadcasted_iota(jnp.int32, (ROWS, LANES), 1) // GROUP

    def sweep(level, tile, pack, spot):
        base = FIRST + tile * ROWS

        def at(field, shift):
            return pad[field, level, pl.ds(base + shift, ROWS), :]

        wet = at(count + 1, 0)
        here = at(count, 0) * at(count + 1, -1) * wet
        after = at(count, 1) * wet * at(count + 1, 1)
        weights = stencil_weights(here, after)
        packed = [None] * (-(-fields // PER))
        for field in range(fields):
            if field < count:
                value = at(field, -2) * weights[0]
                for shift in range(-1, 3):
                    value = value + at(field, shift) * weights[shift + 2]
            elif field == count:
                value = at(count + 2, 0)
            else:
                value = wet
            swept[field, level, pl.ds(tile * ROWS, ROWS), :] = value
            group, place = divmod(field, PER)
            turned = pltpu.roll(value, (GROUP * place + 2) % LANES, 1)
            if place == 0:
                packed[group] = turned
            else:
                packed[group] = jnp.where(lane_group == place, turned, packed[group])
        for group, value in enumerate(packed):
            pack[level, spot, group] = value

    def sides(slot, pack, from_left, from_right):
        to_right = remote(pack, from_left, col_sems, slot, {"ty": right})
        to_left = remote(pack, from_right, col_sems, slot + 1, {"ty": left})
        return to_right, to_left

    has_left, has_right = ty > 0, ty < ty_size - 1

    def start(pair):
        pl.when(has_right)(pair[0].start)
        pl.when(has_left)(pair[1].start)

    def inner_level(level, carry):
        for tile in range(1, tiles - 1):
            sweep(level, tile, pack_in, tile - 1)
        return carry

    lax.fori_loop(0, levels, inner_level, 0)
    early = sides(0, pack_in, left_in, right_in)
    start(early)

    def ecology(level, carry):
        def field(index):
            return pad[index, level, pl.ds(FIRST, along), :]

        wet = field(count + 1)
        depth = jnp.full((along, LANES), -attenuation * (level.astype(jnp.float32) + 0.5), jnp.float32)
        light = sun_buf[...] * jnp.exp(depth)
        inverse = [1.0 / field(j) for j in range(NNUT)]
        recycled = jnp.zeros((along, LANES), jnp.float32)
        for k in range(nphy):
            phyto = field(NNUT + k)
            worst = inverse[0] * half_sat[0, k]
            for j in range(1, NNUT):
                worst = jnp.maximum(worst, inverse[j] * half_sat[j, k])
            growth = growth_max[k] * light * phyto / ((1.0 + worst) * (light + light_half[k]))
            loss = plankton_mortality * phyto
            change = growth - loss
            recycled = recycled - change
            tend[NNUT + k, level] = change
        available = [None] * nzoo
        for k in range(nphy):
            phyto = field(NNUT + k)
            for z in range(nzoo):
                term = prey[z, k] * phyto
                available[z] = term if k == 0 else available[z] + term
        rates = []
        for z in range(nzoo):
            zoo = field(NNUT + nphy + z)
            rate = graze_max[z] * zoo / (graze_half[z] + available[z])
            ingested = rate * available[z]
            loss = grazer_mortality * zoo * zoo
            tend[NNUT + nphy + z, level] = wet * (assimilation * ingested - loss)
            recycled = recycled + loss + (1.0 - assimilation) * ingested
            rates.append(rate)
        for k in range(nphy):
            eaten = prey[0, k] * rates[0]
            for z in range(1, nzoo):
                eaten = eaten + prey[z, k] * rates[z]
            tend[NNUT + k, level] = wet * (tend[NNUT + k, level] - field(NNUT + k) * eaten)
        recycled = wet * recycled
        for j in range(NNUT):
            tend[j, level] = stoichiometry[j] * recycled
        return carry

    lax.fori_loop(0, 1, ecology, 0)

    to_down.wait()
    to_up.wait()
    pad[0:fields, :, FIRST - 2:FIRST, :] = recv_lo[...]
    pad[0:fields, :, FIRST + along:FIRST + along + 2, :] = recv_hi[...]

    def outer_level(level, carry):
        sweep(level, 0, pack_out, 0)
        sweep(level, tiles - 1, pack_out, 1)
        return carry

    lax.fori_loop(0, levels, outer_level, 0)
    late = sides(2, pack_out, left_out, right_out)
    start(late)

    lax.fori_loop(1, levels, ecology, 0)

    @pl.when(jnp.logical_not(has_left))
    def _():
        left_in[...] = jnp.zeros_like(left_in)
        left_out[...] = jnp.zeros_like(left_out)

    @pl.when(jnp.logical_not(has_right))
    def _():
        right_in[...] = jnp.zeros_like(right_in)
        right_out[...] = jnp.zeros_like(right_out)

    for pair in (early, late):
        @pl.when(has_right)
        def _():
            pair[0].wait_send()
            pair[1].wait_recv()

        @pl.when(has_left)
        def _():
            pair[1].wait_send()
            pair[0].wait_recv()

    lane = lax.broadcasted_iota(jnp.int32, left_in.shape[-2:], 1)
    from_left = (lane % GROUP) < 2
    halo[:, 1:tiles - 1] = jnp.where(from_left, left_in[...], right_in[...])
    edge = jnp.where(from_left, left_out[...], right_out[...])
    halo[:, 0] = edge[:, 0]
    halo[:, tiles - 1] = edge[:, 1]


def across_kernel(dims, swept, tend, halo, updated, result, sems):
    count, levels, along = dims
    tiles = along // ROWS
    lane = lax.broadcasted_iota(jnp.int32, (ROWS, LANES), 1)
    low, high = lane < 2, lane >= LANES - 2
    first, final = lane == 0, lane == LANES - 1
    copies = []
    for level in range(levels):
        def step(tile, carry):
            rows = pl.ds(pl.multiple_of(tile * ROWS, ROWS), ROWS)
            packs = [halo[level, tile, g] for g in range(halo.shape[2])]

            def parts(field):
                group, place = divmod(field, PER)
                value = swept[field, level, rows, :]
                ends = pltpu.roll(packs[group], (-GROUP * place - 2) % LANES, 1)
                return value, ends

            def below(value, ends):
                return pltpu.roll(jnp.where(final, ends, value), 1, 1)

            def above(value, ends):
                return pltpu.roll(jnp.where(first, ends, value), LANES - 1, 1)

            flow, flow_ends = parts(count)
            wet, wet_ends = parts(count + 1)
            here = flow * below(wet, wet_ends) * wet
            after = above(flow, flow_ends) * wet * above(wet, wet_ends)
            weights = stencil_weights(here, after)
            for field in range(count):
                value, ends = parts(field)
                before, behind = jnp.where(high, ends, value), jnp.where(low, ends, value)
                total = tend[field, level, rows, :] + value * weights[2]
                total = total + pltpu.roll(before, 2, 1) * weights[0]
                total = total + below(value, ends) * weights[1]
                total = total + above(value, ends) * weights[3]
                total = total + pltpu.roll(behind, LANES - 2, 1) * weights[4]
                result[field, level, rows, :] = total
            return carry

        lax.fori_loop(0, tiles, step, 0)
        copy = pltpu.make_async_copy(result.at[:, level], updated.at[:, level], sems.at[level])
        copy.start()
        copies.append(copy)
    for copy in copies:
        copy.wait()


def shards(
    tracers,
    velocity,
    land_mask,
    sunlight,
    growth_max,
    half_sat,
    light_half,
    graze_max,
    graze_half,
    palatable,
    stoichiometry,
):
    count, levels, along, across = tracers.shape
    assert across == LANES and along % ROWS == 0 and along >= 3 * ROWS
    nphy, nzoo = growth_max.shape[0], graze_max.shape[0]
    fields = count + 2
    groups = -(-fields // PER)
    tiles = along // ROWS
    f32 = jnp.float32
    any_space = pl.BlockSpec(memory_space=pl.ANY)
    vmem = pl.BlockSpec(memory_space=pltpu.VMEM)
    smem = pl.BlockSpec(memory_space=pltpu.SMEM)
    inner_shape = (levels, tiles - 2, groups, ROWS, LANES)
    outer_shape = (levels, 2, groups, ROWS, LANES)
    edge = (fields, levels, 2, LANES)
    swept, tend, halo = pl.pallas_call(
        functools.partial(exchange_kernel, (count, levels, along, nphy, nzoo)),
        out_shape=(
            jax.ShapeDtypeStruct((fields, levels, along, across), f32),
            jax.ShapeDtypeStruct(tracers.shape, f32),
            jax.ShapeDtypeStruct((levels, tiles, groups, ROWS, LANES), f32),
        ),
        in_specs=[any_space] * 4 + [smem] * 7,
        out_specs=(vmem, vmem, vmem),
        scratch_shapes=[
            pltpu.VMEM((count + 3, levels, FIRST + along + ROWS, LANES), f32),
            pltpu.VMEM(land_mask.shape, jnp.int32),
            pltpu.VMEM(sunlight.shape, f32),
            pltpu.VMEM(edge, f32),
            pltpu.VMEM(edge, f32),
            pltpu.VMEM(edge, f32),
            pltpu.VMEM(edge, f32),
            pltpu.VMEM(inner_shape, f32),
            pltpu.VMEM(outer_shape, f32),
            pltpu.VMEM(inner_shape, f32),
            pltpu.VMEM(outer_shape, f32),
            pltpu.VMEM(inner_shape, f32),
            pltpu.VMEM(outer_shape, f32),
            pltpu.SMEM(palatable.shape, f32),
            pltpu.SemaphoreType.DMA((7,)),
            pltpu.SemaphoreType.DMA((2, 2)),
            pltpu.SemaphoreType.DMA((4, 2)),
        ],
        compiler_params=pltpu.CompilerParams(
            collective_id=0, has_side_effects=True, vmem_limit_bytes=24 * 2**20
        ),
        name="exchange",
    )(
        tracers, velocity, land_mask, sunlight, growth_max, half_sat, light_half,
        graze_max, graze_half, palatable, stoichiometry,
    )
    return pl.pallas_call(
        functools.partial(across_kernel, (count, levels, along)),
        out_shape=jax.ShapeDtypeStruct(tracers.shape, f32),
        in_specs=[vmem] * 3,
        out_specs=any_space,
        scratch_shapes=[pltpu.VMEM(tracers.shape, f32), pltpu.SemaphoreType.DMA((levels,))],
        compiler_params=pltpu.CompilerParams(vmem_limit_bytes=24 * 2**20),
        name="across",
    )(swept, tend, halo)


def solution(mesh):
    return jax.shard_map(
        shards,
        mesh=mesh,
        in_specs=(
            P("member", None, "tx", "ty"),
            P(None, None, "tx", "ty"),
            P(None, "tx", "ty"),
            P("tx", "ty"),
            P("member"),
            P("member", None),
            P("member"),
            P("member"),
            P("member"),
            P("member", None),
            P(),
        ),
        out_specs=P("member", None, "tx", "ty"),
        check_vma=False,
    )
```

```python
import functools

import jax
import jax.numpy as jnp
from jax import lax
from jax.experimental import pallas as pl
from jax.experimental.pallas import tpu as pltpu
from jax.sharding import PartitionSpec as P

NNUT = 4
plankton_mortality = 0.05
grazer_mortality = 0.3
assimilation = 0.3
attenuation = 0.4

ROWS = 8
LANES = 128
FIRST = 8
GROUP = 4
PER = LANES // GROUP
BATCH = 8
MESH = pl.DeviceIdType.MESH


def stencil_weights(here, after):
    hp, hm = jnp.maximum(here, 0.0), jnp.minimum(here, 0.0)
    ap, am = jnp.maximum(after, 0.0), jnp.minimum(after, 0.0)
    sixth = 1.0 / 6.0
    return (
        -sixth * hp,
        5.0 * sixth * hp + 2.0 * sixth * hm + sixth * ap,
        1.0 - 4.0 * sixth * hp - sixth * hm + sixth * ap + 4.0 * sixth * am,
        -sixth * hm - 2.0 * sixth * ap - 5.0 * sixth * am,
        sixth * am,
    )


def exchange_kernel(
    dims,
    tracers,
    velocity,
    land_mask,
    sunlight,
    *refs,
):
    sources, (swept, tend, halo), tables, buffers = refs[:7], refs[7:10], refs[10:17], refs[17:]
    growth_max, half_sat, light_half, graze_max, graze_half, palatable, stoichiometry = tables
    (
    pad,
    mask_buf,
    sun_buf,
    send_lo,
    send_hi,
    recv_lo,
    recv_hi,
    pack_in,
    pack_out,
    left_in,
    left_out,
    right_in,
    right_out,
    prey,
    load_sems,
    row_sems,
    col_sems,
    ) = buffers
    count, levels, along, nphy, nzoo = dims
    fields = count + 2
    tiles = along // ROWS
    inner = tiles - 2
    last = FIRST + along - ROWS
    tx_size, ty_size = lax.axis_size("tx"), lax.axis_size("ty")
    tx, ty = lax.axis_index("tx"), lax.axis_index("ty")
    up, down = lax.rem(tx + 1, tx_size), lax.rem(tx + tx_size - 1, tx_size)
    right, left = lax.rem(ty + 1, ty_size), lax.rem(ty + ty_size - 1, ty_size)

    def load(slot, src, dst):
        copy = pltpu.make_async_copy(src, dst, load_sems.at[slot])
        copy.start()
        return copy

    own = pl.ds(0, count)
    loads = [
        load(0, land_mask, mask_buf),
        load(1, velocity.at[0], pad.at[count, :, pl.ds(FIRST, along), :]),
        load(2, tracers.at[:, :, pl.ds(0, ROWS), :], pad.at[own, :, pl.ds(FIRST, ROWS), :]),
        load(3, tracers.at[:, :, pl.ds(along - ROWS, ROWS), :], pad.at[own, :, pl.ds(last, ROWS), :]),
        load(4, tracers.at[:, :, pl.ds(ROWS, along - 2 * ROWS), :],
             pad.at[own, :, pl.ds(FIRST + ROWS, along - 2 * ROWS), :]),
        load(5, velocity.at[1], pad.at[count + 2, :, pl.ds(FIRST, along), :]),
        load(6, sunlight, sun_buf),
    ]
    small = [load(7 + i, src, dst) for i, (src, dst) in enumerate(zip(sources, tables))]

    barrier = pltpu.get_barrier_semaphore()
    for target in ({"tx": up}, {"tx": down}, {"ty": right}, {"ty": left}):
        pl.semaphore_signal(barrier, inc=1, device_id=target, device_id_type=MESH)

    def to_float(z, carry):
        for k in range(nphy):
            prey[z, k] = palatable[z, k].astype(jnp.float32)
        return carry

    for copy in small:
        copy.wait()
    lax.fori_loop(0, nzoo, to_float, 0)

    loads[0].wait()
    pad[count + 1, :, FIRST:FIRST + along, :] = mask_buf[...].astype(jnp.float32)
    for slot in (1, 2, 3):
        loads[slot].wait()
    send_lo[...] = pad[0:fields, :, FIRST:FIRST + 2, :]
    send_hi[...] = pad[0:fields, :, FIRST + along - 2:FIRST + along, :]

    pl.semaphore_wait(barrier, 4)

    def remote(src, dst, sems, slot, target):
        return pltpu.make_async_remote_copy(
            src_ref=src, dst_ref=dst, send_sem=sems.at[slot, 0], recv_sem=sems.at[slot, 1],
            device_id=target, device_id_type=MESH,
        )

    to_down = remote(send_lo, recv_hi, row_sems, 0, {"tx": down})
    to_up = remote(send_hi, recv_lo, row_sems, 1, {"tx": up})
    to_down.start()
    to_up.start()
    for slot in (4, 5, 6):
        loads[slot].wait()

    lane_group = lax.broadcasted_iota(jnp.int32, (ROWS, LANES), 1) // GROUP

    def sweep(level, tile, pack, spot):
        base = FIRST + tile * ROWS

        def at(field, shift):
            return pad[field, level, pl.ds(base + shift, ROWS), :]

        wet = at(count + 1, 0)
        here = at(count, 0) * at(count + 1, -1) * wet
        after = at(count, 1) * wet * at(count + 1, 1)
        weights = stencil_weights(here, after)
        packed = [None] * (-(-fields // PER))
        for begin in range(0, fields, BATCH):
            batch = range(begin, min(begin + BATCH, fields))
            values = []
            for field in batch:
                if field < count:
                    value = at(field, -2) * weights[0]
                    for shift in range(-1, 3):
                        value = value + at(field, shift) * weights[shift + 2]
                elif field == count:
                    value = at(count + 2, 0)
                else:
                    value = wet
                values.append(value)
            for field, value in zip(batch, values):
                group, place = divmod(field, PER)
                turned = pltpu.roll(value, (GROUP * place + 2) % LANES, 1)
                if place == 0:
                    packed[group] = turned
                else:
                    packed[group] = jnp.where(lane_group == place, turned, packed[group])
            for field, value in zip(batch, values):
                swept[field, level, pl.ds(tile * ROWS, ROWS), :] = value
        for group, value in enumerate(packed):
            pack[level, spot, group] = value

    def sides(slot, pack, from_left, from_right):
        to_right = remote(pack, from_left, col_sems, slot, {"ty": right})
        to_left = remote(pack, from_right, col_sems, slot + 1, {"ty": left})
        return to_right, to_left

    has_left, has_right = ty > 0, ty < ty_size - 1

    def start(pair):
        pl.when(has_right)(pair[0].start)
        pl.when(has_left)(pair[1].start)

    def inner_level(level, carry):
        for tile in range(1, tiles - 1):
            sweep(level, tile, pack_in, tile - 1)
        return carry

    lax.fori_loop(0, levels, inner_level, 0)
    early = sides(0, pack_in, left_in, right_in)
    start(early)

    def ecology(level, carry):
        def field(index):
            return pad[index, level, pl.ds(FIRST, along), :]

        wet = field(count + 1)
        depth = jnp.full((along, LANES), -attenuation * (level.astype(jnp.float32) + 0.5), jnp.float32)
        light = sun_buf[...] * jnp.exp(depth)
        inverse = [1.0 / field(j) for j in range(NNUT)]
        recycled = jnp.zeros((along, LANES), jnp.float32)
        for k in range(nphy):
            phyto = field(NNUT + k)
            worst = inverse[0] * half_sat[0, k]
            for j in range(1, NNUT):
                worst = jnp.maximum(worst, inverse[j] * half_sat[j, k])
            growth = growth_max[k] * light * phyto / ((1.0 + worst) * (light + light_half[k]))
            loss = plankton_mortality * phyto
            change = growth - loss
            recycled = recycled - change
            tend[NNUT + k, level] = change
        available = [None] * nzoo
        for k in range(nphy):
            phyto = field(NNUT + k)
            for z in range(nzoo):
                term = prey[z, k] * phyto
                available[z] = term if k == 0 else available[z] + term
        rates = []
        for z in range(nzoo):
            zoo = field(NNUT + nphy + z)
            rate = graze_max[z] * zoo / (graze_half[z] + available[z])
            ingested = rate * available[z]
            loss = grazer_mortality * zoo * zoo
            tend[NNUT + nphy + z, level] = wet * (assimilation * ingested - loss)
            recycled = recycled + loss + (1.0 - assimilation) * ingested
            rates.append(rate)
        for k in range(nphy):
            eaten = prey[0, k] * rates[0]
            for z in range(1, nzoo):
                eaten = eaten + prey[z, k] * rates[z]
            tend[NNUT + k, level] = wet * (tend[NNUT + k, level] - field(NNUT + k) * eaten)
        recycled = wet * recycled
        for j in range(NNUT):
            tend[j, level] = stoichiometry[j] * recycled
        return carry

    lax.fori_loop(0, 1, ecology, 0)

    to_down.wait()
    to_up.wait()
    pad[0:fields, :, FIRST - 2:FIRST, :] = recv_lo[...]
    pad[0:fields, :, FIRST + along:FIRST + along + 2, :] = recv_hi[...]

    def outer_level(level, carry):
        sweep(level, 0, pack_out, 0)
        sweep(level, tiles - 1, pack_out, 1)
        return carry

    lax.fori_loop(0, levels, outer_level, 0)
    late = sides(2, pack_out, left_out, right_out)
    start(late)

    lax.fori_loop(1, levels, ecology, 0)

    @pl.when(jnp.logical_not(has_left))
    def _():
        left_in[...] = jnp.zeros_like(left_in)
        left_out[...] = jnp.zeros_like(left_out)

    @pl.when(jnp.logical_not(has_right))
    def _():
        right_in[...] = jnp.zeros_like(right_in)
        right_out[...] = jnp.zeros_like(right_out)

    for pair in (early, late):
        @pl.when(has_right)
        def _():
            pair[0].wait_send()
            pair[1].wait_recv()

        @pl.when(has_left)
        def _():
            pair[1].wait_send()
            pair[0].wait_recv()

    lane = lax.broadcasted_iota(jnp.int32, left_in.shape[-2:], 1)
    from_left = (lane % GROUP) < 2
    halo[:, 1:tiles - 1] = jnp.where(from_left, left_in[...], right_in[...])
    edge = jnp.where(from_left, left_out[...], right_out[...])
    halo[:, 0] = edge[:, 0]
    halo[:, tiles - 1] = edge[:, 1]


def across_kernel(dims, swept, tend, halo, updated, result, sems):
    count, levels, along = dims
    tiles = along // ROWS
    lane = lax.broadcasted_iota(jnp.int32, (ROWS, LANES), 1)
    low, high = lane < 2, lane >= LANES - 2
    first, final = lane == 0, lane == LANES - 1
    copies = []
    for level in range(levels):
        def step(tile, carry):
            rows = pl.ds(pl.multiple_of(tile * ROWS, ROWS), ROWS)
            packs = [halo[level, tile, g] for g in range(halo.shape[2])]

            def parts(field):
                group, place = divmod(field, PER)
                value = swept[field, level, rows, :]
                ends = pltpu.roll(packs[group], (-GROUP * place - 2) % LANES, 1)
                return value, ends

            def below(value, ends):
                return pltpu.roll(jnp.where(final, ends, value), 1, 1)

            def above(value, ends):
                return pltpu.roll(jnp.where(first, ends, value), LANES - 1, 1)

            flow, flow_ends = parts(count)
            wet, wet_ends = parts(count + 1)
            here = flow * below(wet, wet_ends) * wet
            after = above(flow, flow_ends) * wet * above(wet, wet_ends)
            weights = stencil_weights(here, after)
            for begin in range(0, count, BATCH):
                batch = range(begin, min(begin + BATCH, count))
                pairs = [parts(field) for field in batch]
                far_before = [pltpu.roll(jnp.where(high, e, v), 2, 1) for v, e in pairs]
                near_before = [below(v, e) for v, e in pairs]
                near_behind = [above(v, e) for v, e in pairs]
                far_behind = [pltpu.roll(jnp.where(low, e, v), LANES - 2, 1) for v, e in pairs]
                totals = []
                for i, field in enumerate(batch):
                    total = tend[field, level, rows, :] + pairs[i][0] * weights[2]
                    total = total + far_before[i] * weights[0] + near_before[i] * weights[1]
                    total = total + near_behind[i] * weights[3] + far_behind[i] * weights[4]
                    totals.append(total)
                for i, field in enumerate(batch):
                    result[field, level, rows, :] = totals[i]
            return carry

        lax.fori_loop(0, tiles, step, 0)
        copy = pltpu.make_async_copy(result.at[:, level], updated.at[:, level], sems.at[level])
        copy.start()
        copies.append(copy)
    for copy in copies:
        copy.wait()


def shards(
    tracers,
    velocity,
    land_mask,
    sunlight,
    growth_max,
    half_sat,
    light_half,
    graze_max,
    graze_half,
    palatable,
    stoichiometry,
):
    count, levels, along, across = tracers.shape
    assert across == LANES and along % ROWS == 0 and along >= 3 * ROWS
    nphy, nzoo = growth_max.shape[0], graze_max.shape[0]
    fields = count + 2
    groups = -(-fields // PER)
    tiles = along // ROWS
    f32 = jnp.float32
    any_space = pl.BlockSpec(memory_space=pl.ANY)
    hbm = pl.BlockSpec(memory_space=pltpu.HBM)
    vmem = pl.BlockSpec(memory_space=pltpu.VMEM)
    small = (growth_max, half_sat, light_half, graze_max, graze_half, palatable, stoichiometry)
    inner_shape = (levels, tiles - 2, groups, ROWS, LANES)
    outer_shape = (levels, 2, groups, ROWS, LANES)
    edge = (fields, levels, 2, LANES)
    swept, tend, halo = pl.pallas_call(
        functools.partial(exchange_kernel, (count, levels, along, nphy, nzoo)),
        out_shape=(
            jax.ShapeDtypeStruct((fields, levels, along, across), f32),
            jax.ShapeDtypeStruct(tracers.shape, f32),
            jax.ShapeDtypeStruct((levels, tiles, groups, ROWS, LANES), f32),
        ),
        in_specs=[hbm] * 11,
        out_specs=(vmem, vmem, vmem),
        scratch_shapes=[pltpu.SMEM(x.shape, x.dtype) for x in small] + [
            pltpu.VMEM((count + 3, levels, FIRST + along + ROWS, LANES), f32),
            pltpu.VMEM(land_mask.shape, jnp.int32),
            pltpu.VMEM(sunlight.shape, f32),
            pltpu.VMEM(edge, f32),
            pltpu.VMEM(edge, f32),
            pltpu.VMEM(edge, f32),
            pltpu.VMEM(edge, f32),
            pltpu.VMEM(inner_shape, f32),
            pltpu.VMEM(outer_shape, f32),
            pltpu.VMEM(inner_shape, f32),
            pltpu.VMEM(outer_shape, f32),
            pltpu.VMEM(inner_shape, f32),
            pltpu.VMEM(outer_shape, f32),
            pltpu.SMEM(palatable.shape, f32),
            pltpu.SemaphoreType.DMA((14,)),
            pltpu.SemaphoreType.DMA((2, 2)),
            pltpu.SemaphoreType.DMA((4, 2)),
        ],
        compiler_params=pltpu.CompilerParams(
            collective_id=0, has_side_effects=True, vmem_limit_bytes=24 * 2**20
        ),
        name="exchange",
    )(*[
        pltpu.with_memory_space_constraint(x, pltpu.HBM)
        for x in (tracers, velocity, land_mask, sunlight) + small
    ])
    return pl.pallas_call(
        functools.partial(across_kernel, (count, levels, along)),
        out_shape=jax.ShapeDtypeStruct(tracers.shape, f32),
        in_specs=[vmem] * 3,
        out_specs=any_space,
        scratch_shapes=[pltpu.VMEM(tracers.shape, f32), pltpu.SemaphoreType.DMA((levels,))],
        compiler_params=pltpu.CompilerParams(vmem_limit_bytes=24 * 2**20),
        name="across",
    )(swept, tend, halo)


def solution(mesh):
    return jax.shard_map(
        shards,
        mesh=mesh,
        in_specs=(
            P("member", None, "tx", "ty"),
            P(None, None, "tx", "ty"),
            P(None, "tx", "ty"),
            P("tx", "ty"),
            P("member"),
            P("member", None),
            P("member"),
            P("member"),
            P("member"),
            P("member", None),
            P(),
        ),
        out_specs=P("member", None, "tx", "ty"),
        check_vma=False,
    )
```

```python
import functools

import jax
import jax.numpy as jnp
from jax import lax
from jax.experimental import pallas as pl
from jax.experimental.pallas import tpu as pltpu
from jax.sharding import PartitionSpec as P

NNUT = 4
plankton_mortality = 0.05
grazer_mortality = 0.3
assimilation = 0.3
attenuation = 0.4

ROWS = 8
LANES = 128
FIRST = 8
GROUP = 4
PER = LANES // GROUP
BATCH = 8
MESH = pl.DeviceIdType.MESH


def stencil_weights(here, after):
    hp, hm = jnp.maximum(here, 0.0), jnp.minimum(here, 0.0)
    ap, am = jnp.maximum(after, 0.0), jnp.minimum(after, 0.0)
    sixth = 1.0 / 6.0
    return (
        -sixth * hp,
        5.0 * sixth * hp + 2.0 * sixth * hm + sixth * ap,
        1.0 - 4.0 * sixth * hp - sixth * hm + sixth * ap + 4.0 * sixth * am,
        -sixth * hm - 2.0 * sixth * ap - 5.0 * sixth * am,
        sixth * am,
    )


def exchange_kernel(
    dims,
    tracers,
    velocity,
    land_mask,
    sunlight,
    *refs,
):
    sources, (swept, tend, halo), tables, buffers = refs[:7], refs[7:10], refs[10:17], refs[17:]
    growth_max, half_sat, light_half, graze_max, graze_half, palatable, stoichiometry = tables
    (
    pad,
    mask_buf,
    sun_buf,
    send_lo,
    send_hi,
    recv_lo,
    recv_hi,
    pack_in,
    pack_out,
    left_in,
    left_out,
    right_in,
    right_out,
    prey,
    load_sems,
    row_sems,
    col_sems,
    ) = buffers
    count, levels, along, nphy, nzoo = dims
    fields = count + 2
    tiles = along // ROWS
    inner = tiles - 2
    last = FIRST + along - ROWS
    tx_size, ty_size = lax.axis_size("tx"), lax.axis_size("ty")
    tx, ty = lax.axis_index("tx"), lax.axis_index("ty")
    up, down = lax.rem(tx + 1, tx_size), lax.rem(tx + tx_size - 1, tx_size)
    right, left = lax.rem(ty + 1, ty_size), lax.rem(ty + ty_size - 1, ty_size)

    def load(slot, src, dst):
        copy = pltpu.make_async_copy(src, dst, load_sems.at[slot])
        copy.start()
        return copy

    own = pl.ds(0, count)
    loads = [
        load(0, land_mask, mask_buf),
        load(1, velocity.at[0], pad.at[count, :, pl.ds(FIRST, along), :]),
        load(2, tracers.at[:, :, pl.ds(0, ROWS), :], pad.at[own, :, pl.ds(FIRST, ROWS), :]),
        load(3, tracers.at[:, :, pl.ds(along - ROWS, ROWS), :], pad.at[own, :, pl.ds(last, ROWS), :]),
        load(4, tracers.at[:, :, pl.ds(ROWS, along - 2 * ROWS), :],
             pad.at[own, :, pl.ds(FIRST + ROWS, along - 2 * ROWS), :]),
        load(5, velocity.at[1], pad.at[count + 2, :, pl.ds(FIRST, along), :]),
        load(6, sunlight, sun_buf),
    ]
    small = [load(7 + i, src, dst) for i, (src, dst) in enumerate(zip(sources, tables))]

    barrier = pltpu.get_barrier_semaphore()
    for target in ({"tx": up}, {"tx": down}, {"ty": right}, {"ty": left}):
        pl.semaphore_signal(barrier, inc=1, device_id=target, device_id_type=MESH)

    def to_float(z, carry):
        for k in range(nphy):
            prey[z, k] = palatable[z, k].astype(jnp.float32)
        return carry

    for copy in small:
        copy.wait()
    lax.fori_loop(0, nzoo, to_float, 0)

    loads[0].wait()
    pad[count + 1, :, FIRST:FIRST + along, :] = mask_buf[...].astype(jnp.float32)
    for slot in (1, 2, 3):
        loads[slot].wait()
    send_lo[...] = pad[0:fields, :, FIRST:FIRST + 2, :]
    send_hi[...] = pad[0:fields, :, FIRST + along - 2:FIRST + along, :]

    pl.semaphore_wait(barrier, 4)

    def remote(src, dst, sems, slot, target):
        return pltpu.make_async_remote_copy(
            src_ref=src, dst_ref=dst, send_sem=sems.at[slot, 0], recv_sem=sems.at[slot, 1],
            device_id=target, device_id_type=MESH,
        )

    to_down = remote(send_lo, recv_hi, row_sems, 0, {"tx": down})
    to_up = remote(send_hi, recv_lo, row_sems, 1, {"tx": up})
    to_down.start()
    to_up.start()
    for slot in (4, 5, 6):
        loads[slot].wait()

    lane_group = lax.broadcasted_iota(jnp.int32, (ROWS, LANES), 1) // GROUP

    def sweep(level, tile, pack, spot):
        base = FIRST + tile * ROWS

        def at(field, shift):
            return pad[field, level, pl.ds(base + shift, ROWS), :]

        wet = at(count + 1, 0)
        here = at(count, 0) * at(count + 1, -1) * wet
        after = at(count, 1) * wet * at(count + 1, 1)
        weights = stencil_weights(here, after)
        packed = [None] * (-(-fields // PER))
        for begin in range(0, fields, BATCH):
            batch = range(begin, min(begin + BATCH, fields))
            values = []
            for field in batch:
                if field < count:
                    value = at(field, -2) * weights[0]
                    for shift in range(-1, 3):
                        value = value + at(field, shift) * weights[shift + 2]
                elif field == count:
                    value = at(count + 2, 0)
                else:
                    value = wet
                values.append(value)
            for field, value in zip(batch, values):
                group, place = divmod(field, PER)
                turned = pltpu.roll(value, (GROUP * place + 2) % LANES, 1)
                if place == 0:
                    packed[group] = turned
                else:
                    packed[group] = jnp.where(lane_group == place, turned, packed[group])
            for field, value in zip(batch, values):
                swept[field, level, pl.ds(tile * ROWS, ROWS), :] = value
        for group, value in enumerate(packed):
            pack[level, spot, group] = value

    def sides(slot, pack, from_left, from_right):
        to_right = remote(pack, from_left, col_sems, slot, {"ty": right})
        to_left = remote(pack, from_right, col_sems, slot + 1, {"ty": left})
        return to_right, to_left

    has_left, has_right = ty > 0, ty < ty_size - 1

    def start(pair):
        pl.when(has_right)(pair[0].start)
        pl.when(has_left)(pair[1].start)

    def inner_level(level, carry):
        for tile in range(1, tiles - 1):
            sweep(level, tile, pack_in, tile - 1)
        return carry

    lax.fori_loop(0, levels, inner_level, 0)
    early = sides(0, pack_in, left_in, right_in)
    start(early)

    def ecology(level, carry):
        def field(index):
            return pad[index, level, pl.ds(FIRST, along), :]

        wet = field(count + 1)
        depth = jnp.full((along, LANES), -attenuation * (level.astype(jnp.float32) + 0.5), jnp.float32)
        light = sun_buf[...] * jnp.exp(depth)
        inverse = [1.0 / field(j) for j in range(NNUT)]
        recycled = jnp.zeros((along, LANES), jnp.float32)
        for k in range(nphy):
            phyto = field(NNUT + k)
            worst = inverse[0] * half_sat[0, k]
            for j in range(1, NNUT):
                worst = jnp.maximum(worst, inverse[j] * half_sat[j, k])
            growth = growth_max[k] * light * phyto / ((1.0 + worst) * (light + light_half[k]))
            loss = plankton_mortality * phyto
            change = growth - loss
            recycled = recycled - change
            tend[NNUT + k, level] = change
        available = [None] * nzoo
        for k in range(nphy):
            phyto = field(NNUT + k)
            for z in range(nzoo):
                term = prey[z, k] * phyto
                available[z] = term if k == 0 else available[z] + term
        rates = []
        for z in range(nzoo):
            zoo = field(NNUT + nphy + z)
            rate = graze_max[z] * zoo / (graze_half[z] + available[z])
            ingested = rate * available[z]
            loss = grazer_mortality * zoo * zoo
            tend[NNUT + nphy + z, level] = wet * (assimilation * ingested - loss)
            recycled = recycled + loss + (1.0 - assimilation) * ingested
            rates.append(rate)
        for k in range(nphy):
            eaten = prey[0, k] * rates[0]
            for z in range(1, nzoo):
                eaten = eaten + prey[z, k] * rates[z]
            tend[NNUT + k, level] = wet * (tend[NNUT + k, level] - field(NNUT + k) * eaten)
        recycled = wet * recycled
        for j in range(NNUT):
            tend[j, level] = stoichiometry[j] * recycled
        return carry

    lax.fori_loop(0, levels, ecology, 0)

    to_down.wait()
    to_up.wait()
    pad[0:fields, :, FIRST - 2:FIRST, :] = recv_lo[...]
    pad[0:fields, :, FIRST + along:FIRST + along + 2, :] = recv_hi[...]

    def outer_level(level, carry):
        sweep(level, 0, pack_out, 0)
        sweep(level, tiles - 1, pack_out, 1)
        return carry

    lax.fori_loop(0, levels, outer_level, 0)
    late = sides(2, pack_out, left_out, right_out)
    start(late)

    @pl.when(jnp.logical_not(has_left))
    def _():
        left_in[...] = jnp.zeros_like(left_in)
        left_out[...] = jnp.zeros_like(left_out)

    @pl.when(jnp.logical_not(has_right))
    def _():
        right_in[...] = jnp.zeros_like(right_in)
        right_out[...] = jnp.zeros_like(right_out)

    def finish(pair):
        @pl.when(has_right)
        def _():
            pair[0].wait_send()
            pair[1].wait_recv()

        @pl.when(has_left)
        def _():
            pair[1].wait_send()
            pair[0].wait_recv()

    finish(early)
    lane = lax.broadcasted_iota(jnp.int32, (ROWS, LANES), 1)
    from_left = (lane % GROUP) < 2

    def across_level(level, carry):
        for tile in range(1, tiles - 1):
            packs = [
                jnp.where(from_left, left_in[level, tile - 1, g], right_in[level, tile - 1, g])
                for g in range(halo.shape[2])
            ]
            across_tile(count, level, tile, packs, swept, tend, tend)
        return carry

    lax.fori_loop(0, levels, across_level, 0)
    finish(late)
    halo[...] = jnp.where(from_left, left_out[...], right_out[...])


def across_tile(count, level, tile, packs, swept, tend, result):
    lane = lax.broadcasted_iota(jnp.int32, (ROWS, LANES), 1)
    low, high = lane < 2, lane >= LANES - 2
    first, final = lane == 0, lane == LANES - 1
    rows = pl.ds(tile * ROWS, ROWS)

    def parts(field):
        group, place = divmod(field, PER)
        value = swept[field, level, rows, :]
        ends = pltpu.roll(packs[group], (-GROUP * place - 2) % LANES, 1)
        return value, ends

    def below(value, ends):
        return pltpu.roll(jnp.where(final, ends, value), 1, 1)

    def above(value, ends):
        return pltpu.roll(jnp.where(first, ends, value), LANES - 1, 1)

    flow, flow_ends = parts(count)
    wet, wet_ends = parts(count + 1)
    here = flow * below(wet, wet_ends) * wet
    after = above(flow, flow_ends) * wet * above(wet, wet_ends)
    weights = stencil_weights(here, after)
    for begin in range(0, count, BATCH):
        batch = range(begin, min(begin + BATCH, count))
        pairs = [parts(field) for field in batch]
        far_before = [pltpu.roll(jnp.where(high, e, v), 2, 1) for v, e in pairs]
        near_before = [below(v, e) for v, e in pairs]
        near_behind = [above(v, e) for v, e in pairs]
        far_behind = [pltpu.roll(jnp.where(low, e, v), LANES - 2, 1) for v, e in pairs]
        totals = []
        for i, field in enumerate(batch):
            total = tend[field, level, rows, :] + pairs[i][0] * weights[2]
            total = total + far_before[i] * weights[0] + near_before[i] * weights[1]
            total = total + near_behind[i] * weights[3] + far_behind[i] * weights[4]
            totals.append(total)
        for i, field in enumerate(batch):
            result[field, level, rows, :] = totals[i]


def across_kernel(dims, swept, tend, halo, updated, result, sems):
    count, levels, along = dims
    tiles = along // ROWS
    inner = pl.ds(ROWS, along - 2 * ROWS)
    copies = [pltpu.make_async_copy(tend.at[:, :, inner, :], updated.at[:, :, inner, :], sems.at[0])]
    copies[0].start()
    for spot, tile in enumerate((0, tiles - 1)):
        def step(level, carry):
            packs = [halo[level, spot, g] for g in range(halo.shape[2])]
            across_tile(count, level, tile, packs, swept, tend, result)
            return carry

        lax.fori_loop(0, levels, step, 0)
        rows = pl.ds(tile * ROWS, ROWS)
        copy = pltpu.make_async_copy(result.at[:, :, rows, :], updated.at[:, :, rows, :], sems.at[spot + 1])
        copy.start()
        copies.append(copy)
    for copy in copies:
        copy.wait()


def shards(
    tracers,
    velocity,
    land_mask,
    sunlight,
    growth_max,
    half_sat,
    light_half,
    graze_max,
    graze_half,
    palatable,
    stoichiometry,
):
    count, levels, along, across = tracers.shape
    assert across == LANES and along % ROWS == 0 and along >= 3 * ROWS
    nphy, nzoo = growth_max.shape[0], graze_max.shape[0]
    fields = count + 2
    groups = -(-fields // PER)
    tiles = along // ROWS
    f32 = jnp.float32
    any_space = pl.BlockSpec(memory_space=pl.ANY)
    hbm = pl.BlockSpec(memory_space=pltpu.HBM)
    vmem = pl.BlockSpec(memory_space=pltpu.VMEM)
    small = (growth_max, half_sat, light_half, graze_max, graze_half, palatable, stoichiometry)
    inner_shape = (levels, tiles - 2, groups, ROWS, LANES)
    outer_shape = (levels, 2, groups, ROWS, LANES)
    edge = (fields, levels, 2, LANES)
    swept, tend, halo = pl.pallas_call(
        functools.partial(exchange_kernel, (count, levels, along, nphy, nzoo)),
        out_shape=(
            jax.ShapeDtypeStruct((fields, levels, along, across), f32),
            jax.ShapeDtypeStruct(tracers.shape, f32),
            jax.ShapeDtypeStruct(outer_shape, f32),
        ),
        in_specs=[hbm] * 11,
        out_specs=(vmem, vmem, vmem),
        scratch_shapes=[pltpu.SMEM(x.shape, x.dtype) for x in small] + [
            pltpu.VMEM((count + 3, levels, FIRST + along + ROWS, LANES), f32),
            pltpu.VMEM(land_mask.shape, jnp.int32),
            pltpu.VMEM(sunlight.shape, f32),
            pltpu.VMEM(edge, f32),
            pltpu.VMEM(edge, f32),
            pltpu.VMEM(edge, f32),
            pltpu.VMEM(edge, f32),
            pltpu.VMEM(inner_shape, f32),
            pltpu.VMEM(outer_shape, f32),
            pltpu.VMEM(inner_shape, f32),
            pltpu.VMEM(outer_shape, f32),
            pltpu.VMEM(inner_shape, f32),
            pltpu.VMEM(outer_shape, f32),
            pltpu.SMEM(palatable.shape, f32),
            pltpu.SemaphoreType.DMA((14,)),
            pltpu.SemaphoreType.DMA((2, 2)),
            pltpu.SemaphoreType.DMA((4, 2)),
        ],
        compiler_params=pltpu.CompilerParams(
            collective_id=0, has_side_effects=True, vmem_limit_bytes=24 * 2**20
        ),
        name="exchange",
    )(*[
        pltpu.with_memory_space_constraint(x, pltpu.HBM)
        for x in (tracers, velocity, land_mask, sunlight) + small
    ])
    return pl.pallas_call(
        functools.partial(across_kernel, (count, levels, along)),
        out_shape=jax.ShapeDtypeStruct(tracers.shape, f32),
        in_specs=[vmem] * 3,
        out_specs=any_space,
        scratch_shapes=[pltpu.VMEM(tracers.shape, f32), pltpu.SemaphoreType.DMA((3,))],
        compiler_params=pltpu.CompilerParams(vmem_limit_bytes=24 * 2**20),
        name="across",
    )(swept, tend, halo)


def solution(mesh):
    return jax.shard_map(
        shards,
        mesh=mesh,
        in_specs=(
            P("member", None, "tx", "ty"),
            P(None, None, "tx", "ty"),
            P(None, "tx", "ty"),
            P("tx", "ty"),
            P("member"),
            P("member", None),
            P("member"),
            P("member"),
            P("member"),
            P("member", None),
            P(),
        ),
        out_specs=P("member", None, "tx", "ty"),
        check_vma=False,
    )
```
